32 devices in a mesh: grp: 4 (over y, x), brick: 8 (over z, core).
Axes of the slice: x: 2, y: 2, z: 4, core: 2. Of those that a mesh axis runs over, the one named last changes fastest.
Arguments:
- coeffs: bfloat16 [8, 4096, 1024], P(None, 'brick'), may hold values from -6 to 6
- tensor: bfloat16 [32, 1024, 1024], P('grp', 'brick'), may hold values from -0.005859375 to 0.005859375
- pairs: int32 [2, 2], replicated, may hold values from 0 to 7
- lateral: int32 [4096], P('brick'), may hold values from 0 to 511
- thermal: float32 [8], replicated, may hold values from 0.5 to 1
Outputs:
- updated: float32 [32, 8, 4096], P(None, None, 'brick')
The draws below stay inside these ranges and needn't reach their ends.
Inputs may be any that keep to these rules, and one draw needn't show every extreme that they name: `pairs`: row p names the species that receives the collision term and the species it collides with. A cell's lateral partner, as an index within the same block of 512 cells.
All inputs are finite; a program needn't handle non-finite values.
Results may differ from the reference program's by a relative error of at most 0.0003.
Values may be sent and summed in bfloat16 or wider, within the bound.
A program may use at most 128 MiB of HBM per device.

```python
import math
import jax
import jax.numpy as jnp
from jax import lax

M = 1024
MODES = 32
SPECIES = 8
PAIRS = 2
PLANE = 128
C_DEV = 512
CELLS = 4096


def set_ends(result, stream_key, least, high):
    dims = result.shape
    spot = [jax.random.randint(jax.random.fold_in(stream_key, axis), (), 0, dims[axis]) for axis in range(len(dims))]
    result = result.at[tuple(spot)].set(least)
    longest = dims.index(max(dims))
    spot[longest] = (spot[longest] + 1) % dims[longest]
    return result.at[tuple(spot)].set(high)


def block_levels(rng, shape, shards, least, largest):
    def one(position, blocks):
        draws = jax.random.uniform(jax.random.fold_in(jax.random.fold_in(rng, 6), position), (blocks,), jnp.float32, least / len(shards), largest / len(shards))
        return jnp.repeat(jnp.exp(draws), shape[position] // blocks).reshape((-1,) + (1,) * (len(shape) - position - 1))

    level = one(*shards[0])
    for cut in shards[1:]:
        level = level * one(*cut)
    return level


def bell_draw(own_key, dims, scale, reach, pieces=(), kind=jnp.bfloat16):
    entries = scale * jax.random.normal(own_key, dims, jnp.float32)
    if pieces:
        entries = entries * block_levels(own_key, dims, pieces, -0.22, 0.18)
    return jnp.clip(entries, -reach, reach).astype(kind)


def setup_inputs(seed: int = 0) -> dict:
    arg_keys = jax.random.split(jax.random.key(seed), 6)
    coeffs = bell_draw(arg_keys[0], (SPECIES, CELLS, M), 1.0, 6.0, ((1, 8),))
    tensor = bell_draw(arg_keys[1], (MODES, M, M), (M * M) ** -0.5, 0.005859375, ((0, 4), (1, 8)))
    pairs = set_ends(jax.random.randint(arg_keys[2], (PAIRS, 2), 0, SPECIES), jax.random.fold_in(arg_keys[2], 1), 0, SPECIES - 1).astype(jnp.int32)
    lateral = set_ends(jax.random.randint(arg_keys[3], (CELLS,), 0, C_DEV), jax.random.fold_in(arg_keys[3], 1), 0, C_DEV - 1).astype(jnp.int32)
    thermal = jnp.clip(jnp.exp(jax.random.uniform(arg_keys[4], (SPECIES,), jnp.float32, math.log(0.5), math.log(1.0))), 0.5, 1.0)
    return {"coeffs": coeffs, "tensor": tensor, "pairs": pairs, "lateral": lateral, "thermal": thermal}


collision_update = 0.5
courant = 0.08
max_speed = 11.0
mixing = 0.2

def advance(extended, first_mode, thermal, partner):
    mode_count = extended.shape[0] - 2
    thermo = thermal[None, :, None, None]
    orders = (first_mode + jnp.arange(mode_count, dtype=jnp.int32)).astype(jnp.float32)[:, None, None, None]
    speed = thermo * (jnp.sqrt(orders) * extended[:mode_count] + jnp.sqrt(orders + 1.0) * extended[2:])
    middle = extended[1:mode_count + 1]
    face = 0.5 * (speed[:, :, :-1] + speed[:, :, 1:]) - 0.5 * max_speed * thermo * (middle[:, :, 1:] - middle[:, :, :-1])
    center = middle[:, :, 1:-1]
    shape_flat = (mode_count, center.shape[1], center.shape[2] * center.shape[3])
    center = center.reshape(shape_flat)
    divergence = (face[:, :, 1:] - face[:, :, :-1]).reshape(shape_flat)
    beside = jnp.take(center, partner, axis=2)
    return center - courant * divergence + mixing * (beside - center)

def reference(coeffs, tensor, pairs, lateral, thermal):
    species, cells, width = coeffs.shape
    modes = tensor.shape[0]
    pair_count = pairs.shape[0]
    left_side = coeffs[pairs[:, 0]].astype(jnp.float32).reshape(pair_count * cells, width)
    right_side = coeffs[pairs[:, 1]].astype(jnp.float32).reshape(pair_count * cells, width)

    def one_mode(slab):
        inner = jnp.dot(right_side, slab.astype(jnp.float32).T, precision=lax.Precision.HIGHEST)
        return lax.optimization_barrier(jnp.sum(left_side * inner, axis=1))
    collide = lax.map(one_mode, tensor).reshape(modes, pair_count, cells)
    indicator_matrix = (pairs[:, 0][:, None] == jnp.arange(species, dtype=jnp.int32)[None, :]).astype(jnp.float32)
    collision_operator = jnp.einsum('quw,ut->qtw', collide, indicator_matrix, precision=lax.Precision.HIGHEST)
    brick_window = jnp.transpose(coeffs[:, :, :modes], (2, 0, 1))
    species_state = brick_window.astype(jnp.float32) + collision_update * collision_operator
    species_state = jnp.pad(species_state, ((1, 1), (0, 0), (0, 0)))
    layers = cells // PLANE
    species_state = species_state.reshape(modes + 2, species, layers, PLANE)
    extended = jnp.concatenate([species_state[:, :, -1:], species_state, species_state[:, :, :1]], axis=2)
    cell_index = jnp.arange(cells, dtype=jnp.int32)
    partner = (cell_index // C_DEV * C_DEV + lateral).astype(jnp.int32)
    return advance(extended, jnp.int32(0), thermal, partner)
```

```python
import functools
import math

import jax
import jax.numpy as jnp
from jax import lax
from jax.experimental import pallas as pl
from jax.experimental.pallas import tpu as pltpu
from jax.sharding import PartitionSpec as P

PLANE = 128

collision_update = 0.5
courant = 0.08
max_speed = 11.0
mixing = 0.2


def contract_kernel(t_ref, b_ref, a_ref, o_ref):
    modes, rows, width = t_ref.shape
    inner = jnp.dot(
        t_ref[...].reshape(modes * rows, width), b_ref[...], preferred_element_type=jnp.float32
    )
    factor = a_ref[...].astype(jnp.float32)
    o_ref[...] = jnp.sum(inner.reshape(modes, rows, inner.shape[1]) * factor[None], axis=1)


def contract(slab, right, left):
    modes, rows, width = slab.shape
    count = right.shape[1]
    tile = 512 if count % 512 == 0 else count
    return pl.pallas_call(
        contract_kernel,
        grid=(count // tile,),
        out_shape=jax.ShapeDtypeStruct((modes, count), jnp.float32),
        in_specs=[
            pl.BlockSpec((modes, rows, width), lambda n: (0, 0, 0)),
            pl.BlockSpec((width, tile), lambda n: (0, n)),
            pl.BlockSpec((rows, tile), lambda n: (0, n)),
        ],
        out_specs=pl.BlockSpec((modes, tile), lambda n: (0, n)),
        cost_estimate=pl.CostEstimate(
            flops=2 * modes * rows * width * count,
            bytes_accessed=2 * (modes * rows * width + width * count),
            transcendentals=0,
        ),
        name="contract",
    )(slab, right, left)


def tail_kernel(win_ref, pair_ref, ind_ref, thermo_ref, hot_ref, o_ref, state_ref):
    modes, species, span = win_ref.shape
    pair_count = pair_ref.shape[1]
    cells = o_ref.shape[2]
    thermo = thermo_ref[...]
    zero = jnp.zeros((species, span), jnp.float32)
    for k in range(modes):
        add = zero
        for p in range(pair_count):
            add = add + ind_ref[p] * pair_ref[k, p : p + 1, :]
        state_ref[k] = win_ref[k].astype(jnp.float32) + collision_update * add
    for k in range(modes):
        below = state_ref[k - 1] if k else zero
        above = state_ref[k + 1] if k + 1 < modes else zero
        middle = state_ref[k]
        speed = thermo * (math.sqrt(k) * below + math.sqrt(k + 1.0) * above)
        face = 0.5 * (speed[:, :-PLANE] + speed[:, PLANE:]) - 0.5 * max_speed * thermo * (
            middle[:, PLANE:] - middle[:, :-PLANE]
        )
        center = middle[:, PLANE:-PLANE]
        o_ref[k] = center - courant * (face[:, PLANE:] - face[:, :-PLANE]) - mixing * center
    center = state_ref[:, :, PLANE:-PLANE].reshape(modes * species, cells)
    hot = hot_ref[...]
    top = center.astype(jnp.bfloat16)
    rest = center - top.astype(jnp.float32)
    mid = rest.astype(jnp.bfloat16)
    low = (rest - mid.astype(jnp.float32)).astype(jnp.bfloat16)
    beside = jnp.dot(low, hot, preferred_element_type=jnp.float32)
    beside = beside + jnp.dot(mid, hot, preferred_element_type=jnp.float32)
    beside = beside + jnp.dot(top, hot, preferred_element_type=jnp.float32)
    o_ref[...] += mixing * beside.reshape(modes, species, cells)


def local(coeffs, tensor, pairs, lateral, thermal):
    species, cells, width = coeffs.shape
    local_modes, depth, _ = tensor.shape
    bricks = lax.axis_size("brick")
    modes = local_modes * lax.axis_size("grp")
    pair_count = pairs.shape[0]
    stops = bricks // 2
    me = lax.axis_index("brick")
    core = lax.rem(me, 2)
    spot = me // 2
    half = depth // 2

    onward = [(i, (i + 2) % bricks) for i in range(bricks)]
    back = [((i + 2) % bricks, i) for i in range(bricks)]
    swap = [(i, i ^ 1) for i in range(bricks)]
    up = [(i, (i + 1) % bricks) for i in range(bricks)]
    down = [((i + 1) % bricks, i) for i in range(bricks)]

    low, high = tensor[:, :half], tensor[:, half:]
    arrived = []
    fwd, bwd = (low, high), (low, high)
    for d in range(1, stops // 2 + 1):
        last = 2 * d == stops
        f_low = lax.ppermute(fwd[0], "brick", onward)
        b_high = lax.ppermute(bwd[1], "brick", back)
        arrived += [(-d, 0, f_low), (d, 1, b_high)]
        if not last:
            f_high = lax.ppermute(fwd[1], "brick", onward)
            b_low = lax.ppermute(bwd[0], "brick", back)
            arrived += [(-d, 1, f_high), (d, 0, b_low)]
            fwd, bwd = (f_low, f_high), (b_low, b_high)

    def species_of(column):
        return [
            lax.dynamic_index_in_dim(coeffs, pairs[p, column], axis=0, keepdims=False)
            for p in range(pair_count)
        ]

    right = jnp.concatenate(species_of(1), axis=0).T
    left = jnp.concatenate(species_of(0), axis=0).T.reshape(stops, 2, depth, pair_count * cells)
    mine = lax.dynamic_index_in_dim(left, core, axis=1, keepdims=False)
    other = lax.dynamic_index_in_dim(left, 1 - core, axis=1, keepdims=False)
    right_all = jnp.concatenate([right, lax.ppermute(right, "brick", swap)], axis=1)
    left_all = jnp.concatenate([mine, lax.ppermute(other, "brick", swap)], axis=2)

    window = jnp.transpose(coeffs[:, :, :modes], (2, 0, 1))
    window = jnp.concatenate(
        [
            lax.ppermute(window[:, :, -PLANE:], "brick", up),
            window,
            lax.ppermute(window[:, :, :PLANE], "brick", down),
        ],
        axis=2,
    )
    hot = (jnp.arange(cells, dtype=jnp.int32)[:, None] == lateral[None, :]).astype(jnp.bfloat16)
    indicator = (
        pairs[:, 0][:, None] == jnp.arange(species, dtype=jnp.int32)[None, :]
    ).astype(jnp.float32)[:, :, None]

    total = contract(
        tensor, right_all, lax.dynamic_index_in_dim(left_all, spot, axis=0, keepdims=False)
    )
    for offset, part, slab in arrived:
        owner = lax.rem(spot + offset + stops, stops)
        rows = lax.dynamic_index_in_dim(left_all, owner, axis=0, keepdims=False)
        total = total + contract(slab, right_all, rows[part * half : part * half + half])

    own = pair_count * cells
    collide = total[:, :own] + lax.ppermute(total[:, own:], "brick", swap)
    collide = collide.reshape(local_modes, pair_count, cells)
    pair_all = lax.all_gather(collide, "grp", axis=0, tiled=True)
    pair_all = jnp.concatenate(
        [
            lax.ppermute(pair_all[:, :, -PLANE:], "brick", up),
            pair_all,
            lax.ppermute(pair_all[:, :, :PLANE], "brick", down),
        ],
        axis=2,
    )
    return pl.pallas_call(
        tail_kernel,
        out_shape=jax.ShapeDtypeStruct((modes, species, cells), jnp.float32),
        scratch_shapes=[pltpu.VMEM((modes, species, cells + 2 * PLANE), jnp.float32)],
        name="tail",
    )(window, pair_all, indicator, thermal[:, None], hot)


def solution(mesh):
    in_specs = (P(None, "brick", None), P("grp", "brick", None), P(), P("brick"), P())
    out_specs = P(None, None, "brick")
    return jax.shard_map(local, mesh=mesh, in_specs=in_specs, out_specs=out_specs, check_vma=False)
```

```python
import functools
import math

import jax
import jax.numpy as jnp
from jax import lax
from jax.experimental import pallas as pl
from jax.experimental.pallas import tpu as pltpu
from jax.sharding import PartitionSpec as P

PLANE = 128

collision_update = 0.5
courant = 0.08
max_speed = 11.0
mixing = 0.2


def contract_kernel(t_ref, b_ref, a_ref, o_ref):
    modes, rows, width = t_ref.shape
    inner = jnp.dot(
        t_ref[...].reshape(modes * rows, width), b_ref[...], preferred_element_type=jnp.float32
    )
    factor = a_ref[...].astype(jnp.float32)
    o_ref[...] = jnp.sum(inner.reshape(modes, rows, inner.shape[1]) * factor[None], axis=1)


def contract(slab, right, left):
    modes, rows, width = slab.shape
    count = right.shape[1]
    tile = 512 if count % 512 == 0 else count
    return pl.pallas_call(
        contract_kernel,
        grid=(count // tile,),
        out_shape=jax.ShapeDtypeStruct((modes, count), jnp.float32),
        in_specs=[
            pl.BlockSpec((modes, rows, width), lambda n: (0, 0, 0)),
            pl.BlockSpec((width, tile), lambda n: (0, n)),
            pl.BlockSpec((rows, tile), lambda n: (0, n)),
        ],
        out_specs=pl.BlockSpec((modes, tile), lambda n: (0, n)),
        cost_estimate=pl.CostEstimate(
            flops=2 * modes * rows * width * count,
            bytes_accessed=2 * (modes * rows * width + width * count),
            transcendentals=0,
        ),
        name="contract",
    )(slab, right, left)


def tail_kernel(win_ref, pair_ref, ind_ref, thermo_ref, hot_ref, o_ref, state_ref):
    modes, species, span = win_ref.shape
    pair_count = pair_ref.shape[1]
    cells = o_ref.shape[2]
    thermo = thermo_ref[...]
    zero = jnp.zeros((species, span), jnp.float32)
    for k in range(modes):
        add = zero
        for p in range(pair_count):
            add = add + ind_ref[p] * pair_ref[k, p : p + 1, :]
        state_ref[k] = win_ref[k].astype(jnp.float32) + collision_update * add
    for k in range(modes):
        below = state_ref[k - 1] if k else zero
        above = state_ref[k + 1] if k + 1 < modes else zero
        middle = state_ref[k]
        speed = thermo * (math.sqrt(k) * below + math.sqrt(k + 1.0) * above)
        face = 0.5 * (speed[:, :-PLANE] + speed[:, PLANE:]) - 0.5 * max_speed * thermo * (
            middle[:, PLANE:] - middle[:, :-PLANE]
        )
        center = middle[:, PLANE:-PLANE]
        o_ref[k] = center - courant * (face[:, PLANE:] - face[:, :-PLANE]) - mixing * center
    center = state_ref[:, :, PLANE:-PLANE].reshape(modes * species, cells)
    hot = hot_ref[...]
    top = center.astype(jnp.bfloat16)
    rest = center - top.astype(jnp.float32)
    mid = rest.astype(jnp.bfloat16)
    low = (rest - mid.astype(jnp.float32)).astype(jnp.bfloat16)
    beside = jnp.dot(low, hot, preferred_element_type=jnp.float32)
    beside = beside + jnp.dot(mid, hot, preferred_element_type=jnp.float32)
    beside = beside + jnp.dot(top, hot, preferred_element_type=jnp.float32)
    o_ref[...] += mixing * beside.reshape(modes, species, cells)


def local(coeffs, tensor, pairs, lateral, thermal):
    species, cells, width = coeffs.shape
    local_modes, depth, _ = tensor.shape
    bricks = lax.axis_size("brick")
    groups = lax.axis_size("grp")
    modes = local_modes * groups
    pair_count = pairs.shape[0]
    share = pair_count * cells // groups
    group = lax.axis_index("grp")
    half = depth // 2

    ring = [i ^ (i >> 1) for i in range(groups)]
    if sorted(ring) != list(range(groups)):
        ring = list(range(groups))
    onward = [(ring[i], ring[(i + 1) % groups]) for i in range(groups)]
    back = [(t, s) for s, t in onward]
    up = [(i, (i + 1) % bricks) for i in range(bricks)]
    down = [((i + 1) % bricks, i) for i in range(bricks)]

    arrived = [[] for _ in range(groups)]
    arrived[0].append((0, tensor))
    fwd = bwd = tensor
    for d in range(1, groups // 2 + 1):
        if 2 * d == groups:
            arrived[d].append((0, lax.ppermute(fwd[:, :half], "grp", onward)))
            arrived[d].append((half, lax.ppermute(bwd[:, half:], "grp", back)))
        else:
            fwd = lax.ppermute(fwd, "grp", onward)
            bwd = lax.ppermute(bwd, "grp", back)
            arrived[groups - d].append((0, fwd))
            arrived[d].append((0, bwd))

    def share_of(column):
        rows = jnp.concatenate(
            [
                lax.dynamic_index_in_dim(coeffs, pairs[p, column], axis=0, keepdims=False)
                for p in range(pair_count)
            ],
            axis=0,
        )
        return lax.dynamic_slice_in_dim(rows, group * share, share, axis=0)

    right_all = lax.all_gather(share_of(1), "brick", axis=0, tiled=True).T
    left_all = lax.all_to_all(
        share_of(0).reshape(share, bricks, depth), "brick", 1, 0, tiled=False
    )
    left_all = left_all.reshape(bricks * share, depth).T

    window = jnp.transpose(coeffs[:, :, :modes], (2, 0, 1))
    window = jnp.concatenate(
        [
            lax.ppermute(window[:, :, -PLANE:], "brick", up),
            window,
            lax.ppermute(window[:, :, :PLANE], "brick", down),
        ],
        axis=2,
    )
    hot = (jnp.arange(cells, dtype=jnp.int32)[:, None] == lateral[None, :]).astype(jnp.bfloat16)
    indicator = (
        pairs[:, 0][:, None] == jnp.arange(species, dtype=jnp.int32)[None, :]
    ).astype(jnp.float32)[:, :, None]

    parts = [
        sum(
            contract(slab, right_all, left_all[first : first + slab.shape[1]])
            for first, slab in pieces
        )
        for pieces in arrived
    ]
    total = jnp.stack(parts).reshape(groups * local_modes, bricks, share)
    total = jnp.sum(lax.all_to_all(total, "brick", 1, 0, tiled=False), axis=0)
    total = total.reshape(groups, local_modes, share)
    spots = [ring.index(g) for g in range(groups)]
    spot = sum(jnp.where(group == g, spots[g], 0) for g in range(groups))
    collide = jnp.concatenate(
        [
            lax.dynamic_index_in_dim(
                total, lax.rem(spots[g] - spot + groups, groups), axis=0, keepdims=False
            )
            for g in range(groups)
        ],
        axis=0,
    )
    pair_all = lax.all_gather(collide, "grp", axis=1, tiled=True)
    pair_all = pair_all.reshape(modes, pair_count, cells)
    pair_all = jnp.concatenate(
        [
            lax.ppermute(pair_all[:, :, -PLANE:], "brick", up),
            pair_all,
            lax.ppermute(pair_all[:, :, :PLANE], "brick", down),
        ],
        axis=2,
    )
    return pl.pallas_call(
        tail_kernel,
        out_shape=jax.ShapeDtypeStruct((modes, species, cells), jnp.float32),
        scratch_shapes=[pltpu.VMEM((modes, species, cells + 2 * PLANE), jnp.float32)],
        name="tail",
    )(window, pair_all, indicator, thermal[:, None], hot)


def solution(mesh):
    in_specs = (P(None, "brick", None), P("grp", "brick", None), P(), P("brick"), P())
    out_specs = P(None, None, "brick")
    return jax.shard_map(local, mesh=mesh, in_specs=in_specs, out_specs=out_specs, check_vma=False)
```
